32 devices in a mesh: occ: 4 (over z), vir: 4 (over y, x), ka: 2 (over core).
Axes of the slice: x: 2, y: 2, z: 4, core: 2. Of those that a mesh axis runs over, the one named last changes fastest.
Arguments:
- lambda_amps: bfloat16 [2, 16, 1024, 1024], P(None, 'occ', 'vir', 'ka'), may hold values from -0.25 to 0.25
- screened_ints: bfloat16 [16, 1024, 1024], P(('occ', 'vir'), 'ka'), may hold values from -6 to 6
- half_ints: bfloat16 [16, 1024, 128], P(('occ', 'vir'), 'ka'), may hold values from -0.5 to 0.5
- singles: bfloat16 [128, 1024], P(None, 'vir'), may hold values from -6 to 6
- block_mask: int32 [16, 8, 8], P('occ', 'ka'), may hold values from 0 to 1, as said below
Outputs:
- residual_part: bfloat16 [2, 16, 1024, 1024], P('ka', 'occ', 'vir')
The draws below stay inside these ranges and needn't reach their ends.
Inputs may be any that keep to these rules, and one draw needn't show every extreme that they name: `block_mask`: for each j and each of the 2 equal ranges of e blocks, between 1 and 16 of its 32 blocks are 1; some (j, range) has exactly 16.
All inputs are finite; a program needn't handle non-finite values.
Results may differ from the reference program's by a relative error of at most 0.0058.
Values may be sent and summed in bfloat16 or wider, within the bound.
No kernel may reach another device: no remote copies, remote signals or barrier semaphores. Data moves between devices by JAX's collectives and lax.ppermute only.
A program may use at most 128 MiB of HBM per device.

```python
import jax
import jax.numpy as jnp
from jax import lax

O = 128
V = 1024
TILE = 128
CAP = 16
IW = 2
NB = 8
HALVES = 2
HT = 32
J = 16


def draw_block_mask(key, part):
    first_key, second_key, third_key = jax.random.split(key, 3)
    groups = J * HALVES
    base_draw = jax.random.randint(first_key, (groups,), 1, 6)
    counts = jnp.minimum(base_draw * base_draw, CAP)
    forced = jax.random.randint(second_key, (), 0, groups)
    counts = jnp.where(jnp.arange(groups) == forced, CAP, counts)
    scores = jax.random.randint(third_key, (groups, HT), 0, 1 << 20) * HT + jnp.arange(HT)[None, :]
    ordering = jnp.argsort(scores, axis=1, stable=True)
    ranking = jnp.argsort(ordering, axis=1, stable=True)
    live_tiles = (ranking < counts[:, None]).astype(jnp.int32)
    return live_tiles.reshape(J, NB, NB)


def levels(stream_key, shape, cuts, smallest, largest):
    def one(dim, shards_of):
        heights = jax.random.uniform(jax.random.fold_in(jax.random.fold_in(stream_key, 6), dim), (shards_of,), jnp.float32, smallest / len(cuts), largest / len(cuts))
        return jnp.repeat(jnp.exp(heights), shape[dim] // shards_of).reshape((-1,) + (1,) * (len(shape) - dim - 1))

    factor_of = one(*cuts[0])
    for cut in cuts[1:]:
        factor_of = factor_of * one(*cut)
    return factor_of


def gaussian(own_key, shape, deviation, bound, shards=(), dtype=jnp.bfloat16):
    loudness = levels(own_key, shape, shards, -0.22, 0.18) if shards else 1.0
    values = jax.random.normal(own_key, shape, jnp.float32) * deviation * loudness
    return jnp.minimum(jnp.maximum(values, -bound), bound).astype(dtype)


def setup_inputs(seed: int = 0) -> dict:
    key_list = jax.random.split(jax.random.key(seed), 6)
    return {
        "lambda_amps": gaussian(key_list[0], (IW, J, V, V), (V // 2) ** -0.5, 0.25, ((1, 4), (2, 4), (3, 2))),
        "screened_ints": gaussian(key_list[1], (J, V, V), 1.0, 6.0, ((0, 16), (1, 2))),
        "half_ints": gaussian(key_list[2], (J, V, O), O ** -0.5, 0.5, ((0, 16), (1, 2))),
        "singles": gaussian(key_list[3], (O, V), 1.0, 6.0, ((1, 4),)),
        "block_mask": draw_block_mask(jax.random.fold_in(key_list[5], 71), 0),
    }


def reference(lambda_amps, screened_ints, half_ints, singles, block_mask):
    def per_item(item):
        dressed = screened_ints[item].astype(jnp.float32) - jnp.dot(half_ints[item], singles, preferred_element_type=jnp.float32)
        block_gate = jnp.repeat(jnp.repeat(block_mask[item].astype(jnp.float32), TILE, axis=0), TILE, axis=1)
        blocks = (block_gate * dressed).astype(jnp.bfloat16)
        amp_rows = lambda_amps[:, item].reshape(IW * V, V)
        result = jnp.dot(amp_rows, blocks, preferred_element_type=jnp.float32).astype(jnp.bfloat16)
        return result.reshape(IW, V, V)

    stacked = lax.map(per_item, jnp.arange(J).astype(jnp.int32))
    return jnp.transpose(stacked, (1, 0, 2, 3))
```

```python
import functools

import jax
import jax.numpy as jnp
from jax import lax
from jax.experimental import pallas as pl
from jax.experimental.pallas import tpu as pltpu
from jax.sharding import PartitionSpec as P

TILE = 128
CAP = 16


def pack_kernel(tile, cap, place_ref, mask_ref, x_ref, out_ref, order_ref, sems):
    me = place_ref[0]
    _, row_blocks, col_blocks = mask_ref.shape
    for slot in range(cap + 1):
        order_ref[slot] = 0
    count = jnp.int32(0)
    for row in range(row_blocks):
        for col in range(col_blocks):
            order_ref[count] = row * col_blocks + col
            count = count + mask_ref[me, row, col]
    copies = []
    for slot in range(cap):
        block = order_ref[slot]
        row = pl.multiple_of((block // col_blocks) * tile, tile)
        col = pl.multiple_of((block % col_blocks) * tile, tile)
        copy = pltpu.make_async_copy(
            x_ref.at[0, pl.ds(row, tile), pl.ds(col, tile)], out_ref.at[slot], sems.at[slot]
        )
        copy.start()
        copies.append(copy)
    for copy in copies:
        copy.wait()


def pack(place, block_mask, screened_ints, tile, cap):
    return pl.pallas_call(
        functools.partial(pack_kernel, tile, cap),
        out_shape=jax.ShapeDtypeStruct((cap, tile, tile), screened_ints.dtype),
        in_specs=[
            pl.BlockSpec(memory_space=pltpu.SMEM),
            pl.BlockSpec(memory_space=pltpu.SMEM),
            pl.BlockSpec(memory_space=pl.ANY),
        ],
        out_specs=pl.BlockSpec(memory_space=pltpu.VMEM),
        scratch_shapes=[pltpu.SMEM((cap + 1,), jnp.int32), pltpu.SemaphoreType.DMA((cap,))],
        name="pack",
    )(place, block_mask, screened_ints)


def stage_kernel(tile, aliased, place_ref, own_mask_ref, other_mask_ref, own_amps_ref, other_amps_ref,
                 own_x_ref, other_x_ref, own_y_ref, other_y_ref, t_ref, *rest):
    out_ref, dense_ref = rest[-2:]
    item = place_ref[0]
    t = t_ref[...]
    halves = ((own_mask_ref, own_x_ref, own_y_ref), (other_mask_ref, other_x_ref, other_y_ref))
    for half, (mask_ref, x_ref, y_ref) in enumerate(halves):
        _, row_blocks, col_blocks = mask_ref.shape
        last = x_ref.shape[0] - 1
        count = jnp.int32(0)
        for row in range(row_blocks):
            rows = slice(row * tile, (row + 1) * tile)
            product = jnp.dot(y_ref[0, rows, :], t, preferred_element_type=jnp.float32)
            for col in range(col_blocks):
                cols = slice(col * tile, (col + 1) * tile)
                live = mask_ref[item, row, col]
                block = x_ref[jnp.minimum(count, last)].astype(jnp.float32) - product[:, cols]
                dense_ref[half, rows, cols] = jnp.where(live > 0, block, 0.0).astype(jnp.bfloat16)
                count = count + live
    total = jnp.dot(own_amps_ref[0, 0], dense_ref[0], preferred_element_type=jnp.float32)
    total = total + jnp.dot(other_amps_ref[0, 0], dense_ref[1], preferred_element_type=jnp.float32)
    out_ref[0, 0] = total.astype(out_ref.dtype)


def stage(place, masks, amps, xs, ys, t_all, result, tile):
    own_amps, other_amps = amps
    _, items, rows, half_e = own_amps.shape
    cap = xs[0].shape[0]
    full_b = t_all.shape[1]
    whole = lambda a: pl.BlockSpec(a.shape, lambda g, place: (0,) * a.ndim)
    in_specs = [
        pl.BlockSpec(memory_space=pltpu.SMEM),
        pl.BlockSpec(memory_space=pltpu.SMEM),
        pl.BlockSpec((1, 1, rows, half_e), lambda g, place: (place[1], place[0], 0, 0)),
        pl.BlockSpec((1, 1, rows, half_e), lambda g, place: (0, place[0], 0, 0)),
        whole(xs[0]), whole(xs[1]), whole(ys[0]), whole(ys[1]), whole(t_all),
    ]
    operands = [place, *masks, own_amps, other_amps, *xs, *ys, t_all]
    aliases = {}
    if result is not None:
        in_specs.append(pl.BlockSpec(memory_space=pl.ANY))
        aliases = {len(operands): 0}
        operands.append(result)
    return pl.pallas_call(
        functools.partial(stage_kernel, tile, result is not None),
        out_shape=jax.ShapeDtypeStruct((1, items, rows, full_b), jnp.bfloat16),
        grid_spec=pltpu.PrefetchScalarGridSpec(
            num_scalar_prefetch=1,
            grid=(1,),
            in_specs=in_specs,
            out_specs=pl.BlockSpec((1, 1, rows, full_b), lambda g, place: (0, place[0], 0, 0)),
            scratch_shapes=[pltpu.VMEM((2, half_e, full_b), jnp.bfloat16)],
        ),
        input_output_aliases=aliases,
        name="stage",
    )(*operands)


def compact_body(sizes, lambda_amps, screened_ints, half_ints, singles, block_mask):
    vir, ka = sizes
    tile, cap = TILE, CAP
    me, half = lax.axis_index("vir"), lax.axis_index("ka")
    bits = [1 << k for k in range(vir.bit_length() - 1)]

    def turned(k):
        return bits if k == 0 else bits[::-1]

    def hop(array, b):
        pairs = []
        for v in range(vir):
            for k in range(ka):
                pairs.append((v * ka + k, (v ^ turned(k)[b]) * ka + k))
        return lax.ppermute(array, ("vir", "ka"), pairs)

    def swap(array):
        return lax.ppermute(array, "ka", [(0, 1), (1, 0)])

    def gather(array):
        got = {0: array}
        for b in range(len(bits)):
            for d in list(got):
                got[d | (1 << b)] = hop(got[d], b)
        return got

    def mirrored(d):
        return sum(1 << (len(bits) - 1 - b) for b in range(len(bits)) if d >> b & 1)

    def owner(d):
        first = sum(turned(0)[b] for b in range(len(bits)) if d >> b & 1)
        second = sum(turned(1)[b] for b in range(len(bits)) if d >> b & 1)
        return me ^ jnp.where(half == 0, first, second)

    place = jnp.stack([me, half]).astype(jnp.int32)
    ts = gather(singles)
    ys = gather(half_ints)
    packed = pack(place, block_mask, screened_ints, tile, cap)
    xs = gather(packed)

    other_mask = swap(block_mask)
    other_amps = swap(lax.dynamic_slice_in_dim(lambda_amps, 1 - half, 1, 0))
    width = singles.shape[1]
    t_all = jnp.zeros((singles.shape[0], width * vir), singles.dtype)
    for d in range(vir):
        t_all = lax.dynamic_update_slice(t_all, ts[d], (0, owner(d) * width))
    other_xs = {d: swap(xs[d]) for d in range(vir)}
    other_ys = {d: swap(ys[d]) for d in range(vir)}

    result = None
    for d in range(vir):
        place = jnp.stack([owner(d), half]).astype(jnp.int32)
        e = mirrored(d)
        result = stage(place, (block_mask, other_mask), (lambda_amps, other_amps),
                       (xs[d], other_xs[e]), (ys[d], other_ys[e]), t_all, result, tile)
    return result


def dense_body(lambda_amps, screened_ints, half_ints, singles, block_mask):
    tile = TILE
    single_all = lax.all_gather(singles, "vir", axis=1, tiled=True)
    per_vir, half_rows, full_cols = screened_ints.shape
    own_mask = lax.dynamic_slice_in_dim(block_mask, lax.axis_index("vir") * per_vir, per_vir, 0)
    dressed = screened_ints.astype(jnp.float32) - jnp.einsum(
        "jem,mb->jeb", half_ints, single_all, preferred_element_type=jnp.float32
    )
    gate = jnp.repeat(jnp.repeat(own_mask, tile, axis=1), tile, axis=2).astype(jnp.float32)
    blocks = (dressed * gate).astype(jnp.bfloat16)
    blocks = lax.all_gather(blocks, "vir", axis=0, tiled=True)
    blocks = lax.all_gather(blocks, "ka", axis=1, tiled=True)
    amps = lax.all_to_all(lambda_amps, "ka", split_axis=0, concat_axis=3, tiled=True)
    out = jnp.einsum("ijae,jeb->ijab", amps, blocks, preferred_element_type=jnp.float32)
    return out.astype(jnp.bfloat16)


def body(sizes, lambda_amps, screened_ints, half_ints, singles, block_mask):
    vir, ka = sizes
    args = (lambda_amps, screened_ints, half_ints, singles, block_mask)
    if screened_ints.shape[0] == 1 and ka == 2 and vir > 1 and vir & (vir - 1) == 0:
        return compact_body(sizes, *args)
    return dense_body(*args)


def solution(mesh):
    sizes = mesh.shape["vir"], mesh.shape["ka"]
    return jax.shard_map(
        functools.partial(body, sizes),
        mesh=mesh,
        in_specs=(
            P(None, "occ", "vir", "ka"),
            P(("occ", "vir"), "ka", None),
            P(("occ", "vir"), "ka", None),
            P(None, "vir"),
            P("occ", "ka", None),
        ),
        out_specs=P("ka", "occ", "vir", None),
        check_vma=False,
    )
```

```python
import functools

import jax
import jax.numpy as jnp
from jax import lax
from jax.experimental import pallas as pl
from jax.experimental.pallas import tpu as pltpu
from jax.sharding import PartitionSpec as P

TILE = 128
CAP = 16
VMEM_LIMIT = 16 * 1024 * 1024


def in_vmem(array):
    return pltpu.with_memory_space_constraint(array, pltpu.VMEM)


def vmem_out(shape, dtype):
    return pltpu.VMEM(shape, dtype)


VMEM_SPEC = pl.BlockSpec(memory_space=pltpu.VMEM)
SMEM_SPEC = pl.BlockSpec(memory_space=pltpu.SMEM)


class Grid:
    def __init__(self, vir):
        self.vir = vir
        self.bits = [1 << k for k in range(vir.bit_length() - 1)]

    def offset(self, d, core):
        order = self.bits if core == 0 else self.bits[::-1]
        return sum(bit for k, bit in enumerate(order) if d >> k & 1)

    def owner(self, d):
        me, core = lax.axis_index("vir"), lax.axis_index("ka")
        return me ^ jnp.where(core == 0, self.offset(d, 0), self.offset(d, 1))

    def mirrored(self, d):
        count = len(self.bits)
        return sum(1 << (count - 1 - k) for k in range(count) if d >> k & 1)

    def hop(self, array, k):
        pairs = []
        for v in range(self.vir):
            for core in range(2):
                pairs.append((v * 2 + core, (v ^ self.offset(1 << k, core)) * 2 + core))
        return lax.ppermute(array, ("vir", "ka"), pairs)

    def swap(self, array):
        return lax.ppermute(array, "ka", [(0, 1), (1, 0)])

    def spread(self, got, first):
        got = dict(got)
        for k in range(first, len(self.bits)):
            for d in list(got):
                got[d | (1 << k)] = self.hop(got[d], k)
        return got


def list_live(mask_ref, item, order_ref):
    _, row_blocks, col_blocks = mask_ref.shape
    for slot in range(order_ref.shape[0]):
        order_ref[slot] = 0
    count = jnp.int32(0)
    for row in range(row_blocks):
        for col in range(col_blocks):
            order_ref[count] = row * col_blocks + col
            count = count + mask_ref[item, row, col]


def pack_kernel(tile, mask_ref, x_ref, out_ref, order_ref):
    col_blocks = mask_ref.shape[2]
    list_live(mask_ref, lax.axis_index("vir"), order_ref)
    for slot in range(out_ref.shape[0]):
        block = order_ref[slot]
        row = pl.multiple_of((block // col_blocks) * tile, tile)
        col = pl.multiple_of((block % col_blocks) * tile, tile)
        out_ref[slot] = x_ref[0, pl.ds(row, tile), pl.ds(col, tile)]


def pack(block_mask, screened_ints, tile, cap):
    return pl.pallas_call(
        functools.partial(pack_kernel, tile),
        out_shape=vmem_out((cap, tile, tile), screened_ints.dtype),
        in_specs=[SMEM_SPEC, VMEM_SPEC],
        out_specs=VMEM_SPEC,
        scratch_shapes=[pltpu.SMEM((cap + 1,), jnp.int32)],
        compiler_params=pltpu.CompilerParams(vmem_limit_bytes=VMEM_LIMIT),
        name="pack",
    )(block_mask, in_vmem(screened_ints))


def dress_kernel(grid, tile, label, mask_ref, x_ref, y_ref, *rest):
    t_refs, (out_ref, t_ref, order_ref) = rest[:-3], rest[-3:]
    col_blocks = mask_ref.shape[2]
    width = t_refs[0].shape[1]
    for d, piece in enumerate(t_refs):
        if len(t_refs) == 1:
            t_ref[...] = piece[...]
        else:
            t_ref[:, pl.ds(pl.multiple_of(grid.owner(d) * width, tile), width)] = piece[...]
    list_live(mask_ref, grid.owner(label), order_ref)
    for slot in range(out_ref.shape[0]):
        block = order_ref[slot]
        row = pl.multiple_of((block // col_blocks) * tile, tile)
        col = pl.multiple_of((block % col_blocks) * tile, tile)
        product = jnp.dot(y_ref[0, pl.ds(row, tile), :], t_ref[:, pl.ds(col, tile)],
                          preferred_element_type=jnp.float32)
        out_ref[slot] = (x_ref[slot].astype(jnp.float32) - product).astype(out_ref.dtype)


def dress(grid, block_mask, packed, half_ints, t_pieces, tile, label):
    cap = packed.shape[0]
    inner = half_ints.shape[2]
    full_b = sum(piece.shape[1] for piece in t_pieces)
    return pl.pallas_call(
        functools.partial(dress_kernel, grid, tile, label),
        out_shape=vmem_out(packed.shape, packed.dtype),
        in_specs=[SMEM_SPEC] + [VMEM_SPEC] * (2 + len(t_pieces)),
        out_specs=VMEM_SPEC,
        scratch_shapes=[pltpu.VMEM((inner, full_b), half_ints.dtype), pltpu.SMEM((cap + 1,), jnp.int32)],
        compiler_params=pltpu.CompilerParams(vmem_limit_bytes=VMEM_LIMIT),
        name="dress",
    )(block_mask, in_vmem(packed), in_vmem(half_ints), *[in_vmem(piece) for piece in t_pieces])


def place_blocks(tile, mask_ref, item, x_ref, dense_ref):
    _, row_blocks, col_blocks = mask_ref.shape
    last = x_ref.shape[0] - 1
    count = jnp.int32(0)
    for row in range(row_blocks):
        for col in range(col_blocks):
            live = mask_ref[item, row, col]
            block = x_ref[jnp.minimum(count, last)]
            dense_ref[row * tile:(row + 1) * tile, col * tile:(col + 1) * tile] = jnp.where(
                live > 0, block, jnp.zeros_like(block))
            count = count + live


def stage_kernel(grid, tile, label, aliased, own_mask_ref, other_mask_ref, own_amps_ref, other_amps_ref,
                 own_x_ref, other_x_ref, *rest):
    out_ref, dense_ref, rows_ref, sem = rest[-4:]
    item = grid.owner(label)
    place_blocks(tile, own_mask_ref, item, own_x_ref, dense_ref.at[0])
    place_blocks(tile, other_mask_ref, item, other_x_ref, dense_ref.at[1])
    own_amps = own_amps_ref[lax.axis_index("ka"), item]
    other_amps = other_amps_ref[0, item]
    total = jnp.dot(own_amps, dense_ref[0], preferred_element_type=jnp.float32)
    total = total + jnp.dot(other_amps, dense_ref[1], preferred_element_type=jnp.float32)
    rows_ref[...] = total.astype(rows_ref.dtype)
    copy = pltpu.make_async_copy(rows_ref, out_ref.at[0, item], sem)
    copy.start()
    copy.wait()


def stage(grid, masks, amps, xs, result, tile, label):
    own_amps, other_amps = amps
    _, items, rows, half_e = own_amps.shape
    _, row_blocks, col_blocks = masks[0].shape
    full_b = col_blocks * tile
    operands = [*masks, in_vmem(own_amps), in_vmem(other_amps), in_vmem(xs[0]), in_vmem(xs[1])]
    in_specs = [SMEM_SPEC] * 2 + [VMEM_SPEC] * 4
    aliases = {}
    if result is not None:
        in_specs.append(pl.BlockSpec(memory_space=pl.ANY))
        aliases = {len(operands): 0}
        operands.append(result)
    return pl.pallas_call(
        functools.partial(stage_kernel, grid, tile, label, result is not None),
        out_shape=jax.ShapeDtypeStruct((1, items, rows, full_b), own_amps.dtype),
        in_specs=in_specs,
        out_specs=pl.BlockSpec(memory_space=pl.ANY),
        scratch_shapes=[
            pltpu.VMEM((2, half_e, full_b), own_amps.dtype),
            pltpu.VMEM((rows, full_b), own_amps.dtype),
            pltpu.SemaphoreType.DMA,
        ],
        input_output_aliases=aliases,
        compiler_params=pltpu.CompilerParams(vmem_limit_bytes=VMEM_LIMIT),
        name="stage",
    )(*operands)


def compact_body(vir, lambda_amps, screened_ints, half_ints, singles, block_mask):
    tile, cap = TILE, CAP
    grid = Grid(vir)
    t1 = grid.hop(singles, 0)
    y1 = grid.hop(half_ints, 0)
    packed = pack(block_mask, screened_ints, tile, cap)
    c1 = grid.hop(packed, 0)
    if vir == 4:
        ts = {0: singles, 1: t1, 2: grid.swap(t1), 3: grid.hop(t1, 1)}
    else:
        ts = grid.spread({0: singles, 1: t1}, 1)
    width = singles.shape[1]
    if width % tile == 0:
        t_pieces = [ts[d] for d in range(vir)]
    else:
        t_all = jnp.zeros((singles.shape[0], width * vir), singles.dtype)
        for d in range(vir):
            t_all = lax.dynamic_update_slice(t_all, ts[d], (0, grid.owner(d) * width))
        t_pieces = [t_all]

    other_mask = grid.swap(block_mask)
    other_amps = grid.swap(lax.dynamic_slice_in_dim(lambda_amps, 1 - lax.axis_index("ka"), 1, 0))
    xs = {0: dress(grid, block_mask, packed, half_ints, t_pieces, tile, 0)}
    if vir > 1:
        xs[1] = dress(grid, block_mask, c1, y1, t_pieces, tile, 1)
    xs = grid.spread(xs, 1)
    other_xs = {d: grid.swap(xs[d]) for d in range(vir)}
    result = None
    for d in range(vir):
        result = stage(grid, (block_mask, other_mask), (lambda_amps, other_amps),
                       (xs[d], other_xs[grid.mirrored(d)]), result, tile, d)
    return result


def dense_body(lambda_amps, screened_ints, half_ints, singles, block_mask):
    tile = TILE
    single_all = lax.all_gather(singles, "vir", axis=1, tiled=True)
    per_vir, half_rows, full_cols = screened_ints.shape
    own_mask = lax.dynamic_slice_in_dim(block_mask, lax.axis_index("vir") * per_vir, per_vir, 0)
    dressed = screened_ints.astype(jnp.float32) - jnp.einsum(
        "jem,mb->jeb", half_ints, single_all, preferred_element_type=jnp.float32
    )
    gate = jnp.repeat(jnp.repeat(own_mask, tile, axis=1), tile, axis=2).astype(jnp.float32)
    blocks = (dressed * gate).astype(jnp.bfloat16)
    blocks = lax.all_gather(blocks, "vir", axis=0, tiled=True)
    blocks = lax.all_gather(blocks, "ka", axis=1, tiled=True)
    amps = lax.all_to_all(lambda_amps, "ka", split_axis=0, concat_axis=3, tiled=True)
    out = jnp.einsum("ijae,jeb->ijab", amps, blocks, preferred_element_type=jnp.float32)
    return out.astype(jnp.bfloat16)


def body(sizes, *args):
    vir, ka = sizes
    if args[1].shape[0] == 1 and ka == 2 and vir > 1 and vir & (vir - 1) == 0:
        return compact_body(vir, *args)
    return dense_body(*args)


def solution(mesh):
    sizes = mesh.shape["vir"], mesh.shape["ka"]
    return jax.shard_map(
        functools.partial(body, sizes),
        mesh=mesh,
        in_specs=(
            P(None, "occ", "vir", "ka"),
            P(("occ", "vir"), "ka", None),
            P(("occ", "vir"), "ka", None),
            P(None, "vir"),
            P("occ", "ka", None),
        ),
        out_specs=P("ka", "occ", "vir", None),
        check_vma=False,
    )
```
